32 devices in a mesh: grp: 8 (over y, x, core), mem: 4 (over z).
Axes of the slice: x: 2, y: 2, z: 4, core: 2. Of those that a mesh axis runs over, the one named last changes fastest.
Arguments:
- residual: float32 [256, 64, 256], P(('grp', 'mem')), may hold values from -6 to 6
- direction: float32 [256, 64, 256], P(('grp', 'mem')), may hold values from -6 to 6
- local_inverse: bfloat16 [256, 256, 256], P(('grp', 'mem')), may hold values from -1 to 16, as said below
- dirichlet: bfloat16 [256, 256, 256], P(('grp', 'mem')), may hold values from -1 to 16, as said below
- coupling: bfloat16 [256, 24, 256], P(('grp', 'mem')), may hold values from -0.375 to 0.375
- corner_map: int32 [256, 24], P(('grp', 'mem')), may hold values from 0 to 6143
- coarse_factor: bfloat16 [8, 2048, 2048], P('grp'), may hold values from -1 to 3, as said below
Outputs:
- new_residual: float32 [256, 64, 256], P(('grp', 'mem'))
- new_direction: float32 [256, 64, 256], P(('grp', 'mem'))
- step_sizes: float32 [3, 64], replicated
The draws below stay inside these ranges and needn't reach their ends.
Inputs may be any that keep to these rules, and one draw needn't show every extreme that they name: `local_inverse`: each subdomain's matrix is symmetric positive definite. `dirichlet`: each subdomain's matrix is symmetric positive definite. `coarse_factor`: each group's factor is lower triangular with a positive diagonal.
All inputs are finite; a program needn't handle non-finite values.
Results may differ from the reference program's by a relative error of at most 0.0083.
Values sent between devices are 32-bit elements; how exact they have to be, the bound alone decides.
A program may use at most 128 MiB of HBM per device.

```python
import jax
import jax.numpy as jnp
from jax import lax

SUB = 8
NR = 256
NC = 24
Q = 64
NCO = 2048
ITERS = 3
SUBS = 256
N_GRP = 8
N_MEM = 4


def spd_blocks(key, count, order):
    first_key, second_key = jax.random.split(key, 2)
    diagonal = jnp.exp(jax.random.uniform(first_key, (count, order), jnp.float32, jnp.log(1.5), jnp.log(4.0)))
    spread = 0.5 * (3.0 / order) ** 0.5
    raw_values = jax.random.uniform(second_key, (count, order, order), jnp.float32, -spread, spread)
    upper_part = jnp.triu(raw_values, 1)
    matrices = upper_part + jnp.swapaxes(upper_part, 1, 2) + diagonal[:, :, None] * jnp.eye(order, dtype=jnp.float32)
    return matrices


def draw_local_inverse(key, part):
    return spd_blocks(jax.random.fold_in(key, 11), SUBS, NR).astype(jnp.bfloat16)


def draw_dirichlet(key, part):
    return spd_blocks(jax.random.fold_in(key, 12), SUBS, NR).astype(jnp.bfloat16)


def draw_coarse_factor(key, part):
    first_key, second_key = jax.random.split(jax.random.fold_in(key, 13))
    upper_diag = 2.0
    spread = 0.6 * (3.0 / NCO) ** 0.5
    diagonal = jnp.exp(jax.random.uniform(first_key, (N_GRP, NCO), jnp.float32, 0.0, jnp.log(upper_diag)))
    raw_values = jax.random.uniform(second_key, (N_GRP, NCO, NCO), jnp.float32, -spread, spread)
    factor = jnp.tril(raw_values, -1) + diagonal[:, :, None] * jnp.eye(NCO, dtype=jnp.float32)
    return factor.astype(jnp.bfloat16)


def plant(result, stream_key, smallest, largest):
    place = [jax.random.randint(jax.random.fold_in(stream_key, axis), (), 0, length) for axis, length in enumerate(result.shape)]
    longest = result.shape.index(max(result.shape))
    next_to = place[:longest] + [(place[longest] + 1) % result.shape[longest]] + place[longest + 1:]
    return result.at[tuple(place)].set(smallest).at[tuple(next_to)].set(largest)


def block_scale(own_key, dims, shards, smallest, largest):
    loudness, own = 1.0, jax.random.fold_in(own_key, 6)
    for dim, parts in shards:
        steps = jnp.exp(jax.random.uniform(jax.random.fold_in(own, dim), (parts,), jnp.float32, smallest / len(shards), largest / len(shards)))
        loudness = loudness * jnp.repeat(steps, dims[dim] // parts).reshape([-1 if axis == dim else 1 for axis in range(len(dims))])
    return loudness


def normal_values(rng, dims, deviation, limit, cuts=(), held_as=jnp.bfloat16):
    drawn = jax.random.normal(rng, dims, jnp.float32) * deviation
    if len(cuts) > 0:
        drawn = block_scale(rng, dims, cuts, -0.22, 0.18) * drawn
    return jnp.clip(drawn, min=-limit, max=limit).astype(held_as)


def setup_inputs(seed: int = 0) -> dict:
    streams_of = jax.random.split(jax.random.key(seed), 8)
    return {
        "residual": normal_values(streams_of[0], (SUBS, Q, NR), 1.0, 6.0, ((0, 32),), jnp.float32),
        "direction": normal_values(streams_of[1], (SUBS, Q, NR), 1.0, 6.0, ((0, 32),), jnp.float32),
        "local_inverse": draw_local_inverse(jax.random.fold_in(streams_of[7], 71), 0),
        "dirichlet": draw_dirichlet(jax.random.fold_in(streams_of[7], 71), 0),
        "coupling": normal_values(streams_of[4], (SUBS, NC, NR), NR ** -0.5, 0.375, ((0, 32),)),
        "corner_map": plant(jax.random.randint(streams_of[5], (SUBS, NC), 0, 3 * NCO), jax.random.fold_in(streams_of[5], 1), 0, (3 * NCO) - 1).astype(jnp.int32),
        "coarse_factor": draw_coarse_factor(jax.random.fold_in(streams_of[7], 71), 0),
    }


highest = lax.Precision.HIGHEST

def blockwise(matrices, vectors):
    devices = matrices.shape[0] // SUB
    matrix_blocks = matrices.reshape(devices, SUB, NR, NR)
    vector_blocks = vectors.astype(jnp.bfloat16).reshape(devices, SUB, Q, NR)

    def apply_one(operands):
        return jnp.einsum('sij,skj->ski', operands[0].astype(jnp.float32), operands[1].astype(jnp.float32), precision=highest)
    return lax.map(apply_one, (matrix_blocks, vector_blocks)).reshape(vectors.shape)

def coarse_solve(factor, coarse_load):
    forward = jax.scipy.linalg.solve_triangular(factor, coarse_load.T, lower=True)
    return jax.scipy.linalg.solve_triangular(factor, forward, lower=True, trans=1).T

def reference(residual, direction, local_inverse, dirichlet, coupling, corner_map, coarse_factor):
    coupling_wide = coupling.astype(jnp.float32)
    groups = jnp.arange(SUBS, dtype=jnp.int32) // (SUB * N_MEM)
    owner_row = (groups[:, None] + corner_map // NCO - 1) % N_GRP * NCO + corner_map % NCO
    flat_owner = owner_row.reshape(-1).astype(jnp.int32)
    factors = coarse_factor.astype(jnp.float32)
    precond = blockwise(dirichlet, residual)
    norm_now = jnp.sum(residual * precond, axis=(0, 2))
    step_list = []
    for iteration in range(ITERS):
        solved = blockwise(local_inverse, direction)
        partial_value = jnp.einsum('ski,sci->skc', solved, coupling_wide, precision=highest)
        coarse_load = jnp.zeros((Q, N_GRP * NCO), jnp.float32).at[:, flat_owner].add(partial_value.transpose(1, 0, 2).reshape(Q, SUBS * NC))
        blocks = coarse_load.reshape(Q, N_GRP, NCO).transpose(1, 0, 2)
        coarse = lax.map(lambda operands: coarse_solve(operands[0], operands[1]), (factors, blocks))
        coarse = coarse.transpose(1, 0, 2).reshape(Q, N_GRP * NCO)
        picked = coarse[:, flat_owner].reshape(Q, SUBS, NC).transpose(1, 0, 2)
        lifted = jnp.einsum('skc,sci->ski', picked, coupling_wide, precision=highest)
        image = blockwise(local_inverse, direction + lifted)
        curvature = jnp.sum(direction * image, axis=(0, 2))
        alpha = norm_now / curvature
        step_list.append(alpha)
        residual = residual - alpha[None, :, None] * image
        precond = blockwise(dirichlet, residual)
        norm_next = jnp.sum(residual * precond, axis=(0, 2))
        direction = precond + (norm_next / norm_now)[None, :, None] * direction
        norm_now = norm_next
    return (residual, direction, jnp.stack(step_list))
```

```python
import functools

import jax
import jax.numpy as jnp
from jax import lax
from jax.experimental import pallas as pl
from jax.experimental.pallas import tpu as pltpu
from jax.sharding import PartitionSpec as P

ITERS = 3
TILE = 256
MESH = pl.DeviceIdType.MESH
f32, bf16 = jnp.float32, jnp.bfloat16


def nn(a, b):
    return lax.dot_general(a, b, (((1,), (0,)), ((), ())), preferred_element_type=f32)


def nt(a, b):
    return lax.dot_general(a, b, (((1,), (1,)), ((), ())), preferred_element_type=f32)


def split(x):
    high = x.astype(bf16)
    return high, (x - high.astype(f32)).astype(bf16)


def stacked(x):
    return jnp.concatenate(split(x), axis=0)


def folded(x):
    half = x.shape[0] // 2
    return x[:half] + x[half:]


def invert_blocks(factor_ref, inv_high, inv_low):
    count = factor_ref.shape[0] // TILE
    rows = lax.broadcasted_iota(jnp.int32, (TILE, TILE), 0)
    cols = lax.broadcasted_iota(jnp.int32, (TILE, TILE), 1)

    def one(b, carry):
        at = pl.multiple_of(b * TILE, TILE)
        tile = factor_ref[pl.ds(at, TILE), pl.ds(at, TILE)].astype(f32)
        diagonal = jnp.where(rows == cols, tile, 0.0)
        by_row = 1.0 / jnp.sum(diagonal, axis=1, keepdims=True)
        x = jnp.where(rows == cols, by_row, 0.0)
        size = 1
        while size < TILE:
            below = (rows // size == cols // size + 1) & ((rows // size) % 2 == 1)
            c = jnp.where(below, tile, 0.0).astype(bf16)
            xh, xl = split(x)
            t = nn(c, xh) + nn(c, xl)
            th, tl = split(t)
            x = x - (nn(xh, th) + (nn(xh, tl) + nn(xl, th)))
            size *= 2
        xh, xl = split(x)
        inv_high[b] = xh
        inv_low[b] = xl
        return carry

    lax.fori_loop(0, count, one, 0)


def coarse_solve(loads, factor_ref, inv_high, inv_low):
    count = len(loads)

    def part(i, j):
        return factor_ref[i * TILE : (i + 1) * TILE, j * TILE : (j + 1) * TILE]

    loads = list(loads)
    for i in range(count):
        b = stacked(loads[i])
        loads[i] = folded(nt(b, inv_high[i]) + nt(b, inv_low[i]))
        x = stacked(loads[i])
        for j in range(i + 1, count):
            loads[j] = loads[j] - folded(nt(x, part(j, i)))
    for i in reversed(range(count)):
        b = stacked(loads[i])
        loads[i] = folded(nn(b, inv_high[i]) + nn(b, inv_low[i]))
        x = stacked(loads[i])
        for j in reversed(range(i)):
            loads[j] = loads[j] - folded(nn(x, part(i, j)))
    return loads


def kernel(
    n_grp, n_mem,
    res_in, dir_in, linv, dirich, cpad, cmap, factor,
    res, direc, steps,
    pre, image, onehot, inv_high, inv_low,
    cm_recv, p_send, p_recv, k_send, k_recv, sums, norm,
    cm_s, cm_r, p_s, p_r, k_s, k_r, a_s, a_r,
):
    subs, rhs, dofs = res_in.shape
    wide = cpad.shape[1]
    coarse = factor.shape[0]
    lanes = sums.shape[3]
    total = n_grp * n_mem
    slots = 3 * n_mem
    grp, mem = lax.axis_index("grp"), lax.axis_index("mem")
    me = grp * n_mem + mem
    mine = n_mem + mem
    eye = lax.broadcasted_iota(jnp.int32, (rhs, lanes), 0) == lax.broadcasted_iota(jnp.int32, (rhs, lanes), 1)

    def to_row(column):
        return jnp.sum(jnp.where(eye, column, 0.0), axis=0, keepdims=True)

    def to_column(row):
        return jnp.sum(jnp.where(eye, row, 0.0), axis=1, keepdims=True)

    def wait_bytes(ref, *sems):
        for sem in sems:
            pltpu.make_async_copy(ref, ref, sem).wait()

    def to_owners(source, target, send_sem, recv_sem):
        def one(d, carry):
            slot = (mine + d) % slots
            shift, other = slot // n_mem, slot % n_mem
            pltpu.make_async_remote_copy(
                src_ref=source(other), dst_ref=target(shift * n_mem + mem),
                send_sem=send_sem, recv_sem=recv_sem,
                device_id=((grp + shift + n_grp - 1) % n_grp, other), device_id_type=MESH,
            ).start()
            return carry

        lax.fori_loop(1, slots, one, 0)

    def to_users(source, target, send_sem, recv_sem):
        def one(d, carry):
            slot = (mine + d) % slots
            shift, other = slot // n_mem, slot % n_mem
            pltpu.make_async_remote_copy(
                src_ref=source(slot), dst_ref=target(shift * n_mem + mem),
                send_sem=send_sem, recv_sem=recv_sem,
                device_id=((grp + n_grp + 1 - shift) % n_grp, other), device_id_type=MESH,
            ).start()
            return carry

        lax.fori_loop(1, slots, one, 0)

    def sum_start(r, column):
        sums[r, me] = to_row(column)

        def one(d, carry):
            to = (me + d) % total
            pltpu.make_async_remote_copy(
                src_ref=sums.at[r, me], dst_ref=sums.at[r, me],
                send_sem=a_s.at[r], recv_sem=a_r.at[r],
                device_id=(to // n_mem, to % n_mem), device_id_type=MESH,
            ).start()
            return carry

        lax.fori_loop(1, total, one, 0)

    def sum_finish(r):
        wait_bytes(sums.at[r, pl.ds(0, total - 1)], a_s.at[r], a_r.at[r])
        return jnp.sum(sums[r], axis=0)

    def precondition():
        acc = jnp.zeros((rhs, dofs), f32)
        for s in range(subs):
            value = res[s]
            out = nn(value.astype(bf16), dirich[s])
            pre[s] = out
            acc = acc + value * out
        return jnp.sum(acc, axis=1, keepdims=True)

    to_owners(lambda other: cmap, lambda slot: cm_recv.at[slot], cm_s.at[0], cm_r.at[0])
    cm_recv[mine] = cmap[...]
    res[...] = res_in[...]
    direc[...] = dir_in[...]
    sum_start(0, precondition())
    invert_blocks(factor, inv_high, inv_low)
    wait_bytes(cm_recv.at[pl.ds(0, slots - 1)], cm_s.at[0], cm_r.at[0])
    held = onehot.shape[0] == coarse
    place = lax.broadcasted_iota(jnp.int32, (TILE, wide), 0)

    def fill(start, at):
        for slot in range(slots):
            row = cm_recv[slot] - coarse * (slot // n_mem) - start
            onehot[pl.ds(at, TILE), slot * wide : (slot + 1) * wide] = jnp.where(place == row, 1.0, 0.0).astype(bf16)

    def rows_of(i):
        if held:
            return onehot[i * TILE : (i + 1) * TILE, :]
        fill(i * TILE, 0)
        return onehot[...]

    if held:
        def fill_one(i, carry):
            at = pl.multiple_of(i * TILE, TILE)
            fill(at, at)
            return carry

        lax.fori_loop(0, coarse // TILE, fill_one, 0)
    norm[...] = sum_finish(0)

    def iteration(t, carry):
        partial = jnp.zeros((2 * rhs, wide), f32)
        for s in range(subs):
            solved = nn(direc[s].astype(bf16), linv[s])
            partial = partial + nt(stacked(solved), cpad[s])
        p_send[t] = folded(partial).reshape(p_send.shape[1:])
        to_owners(lambda other: p_send.at[t, other], lambda slot: p_recv.at[t, slot], p_s.at[t], p_r.at[t])
        p_recv[t, mine] = p_send[t, mem]
        wait_bytes(p_recv.at[t, pl.ds(0, slots - 1)], p_s.at[t], p_r.at[t])
        packed = jnp.concatenate([stacked(p_recv[t, slot]) for slot in range(slots)], axis=1)
        loads = [folded(nt(packed, rows_of(i))) for i in range(coarse // TILE)]
        loads = coarse_solve(loads, factor, inv_high, inv_low)
        if held:
            packed = jnp.concatenate([stacked(x) for x in loads], axis=1)
            for slot in range(slots):
                k_send[t, slot] = folded(nn(packed, onehot[:, slot * wide : (slot + 1) * wide]))
        else:
            wanted = sum(folded(nn(stacked(x), rows_of(i))) for i, x in enumerate(loads))
            for slot in range(slots):
                k_send[t, slot] = wanted[:, slot * wide : (slot + 1) * wide]
        to_users(lambda slot: k_send.at[t, slot], lambda slot: k_recv.at[t, slot], k_s.at[t], k_r.at[t])
        k_recv[t, mine] = k_send[t, mine]
        wait_bytes(k_recv.at[t, pl.ds(0, slots - 1)], k_s.at[t], k_r.at[t])
        got = k_recv[t].reshape(3, rhs, wide)
        picked = stacked(got[0] + got[1] + got[2])
        acc = jnp.zeros((rhs, dofs), f32)
        for s in range(subs):
            now = direc[s]
            lifted = folded(nn(picked, cpad[s]))
            out = nn((now + lifted).astype(bf16), linv[s])
            image[s] = out
            acc = acc + now * out
        sum_start(2 * t + 1, jnp.sum(acc, axis=1, keepdims=True))
        norm_now = norm[...]
        curvature = sum_finish(2 * t + 1)
        alpha = norm_now / curvature
        steps[t] = alpha
        column = to_column(alpha)
        for s in range(subs):
            res[s] = res[s] - column * image[s]
        sum_start(2 * t + 2, precondition())
        norm_next = sum_finish(2 * t + 2)
        column = to_column(norm_next / norm_now)
        for s in range(subs):
            direc[s] = pre[s] + column * direc[s]
        norm[...] = norm_next
        return carry

    lax.fori_loop(0, steps.shape[0], iteration, 0)


def local(n_grp, n_mem, residual, direction, local_inverse, dirichlet, coupling, corner_map, coarse_factor):
    subs, rhs, dofs = residual.shape
    corners = coupling.shape[1]
    coarse = coarse_factor.shape[1]
    used = subs * corners
    wide = -(-used // TILE) * TILE
    lanes = -(-rhs // 128) * 128
    total, slots, share = n_grp * n_mem, 3 * n_mem, rhs // n_mem
    own = jnp.arange(wide) // corners
    tiled = jnp.pad(jnp.tile(coupling, (1, subs, 1)), ((0, 0), (0, wide - used), (0, 0)))
    cpad = jnp.where(own[None, :, None] == jnp.arange(subs)[:, None, None], tiled, 0).astype(bf16)
    cmap = jnp.pad(corner_map.reshape(1, used), ((0, 0), (0, wide - used)), constant_values=-1)
    vmem = pl.BlockSpec(memory_space=pltpu.VMEM)
    dma = pltpu.SemaphoreType.DMA
    res, direc, steps = pl.pallas_call(
        functools.partial(kernel, n_grp, n_mem),
        out_shape=(
            jax.ShapeDtypeStruct(residual.shape, f32),
            jax.ShapeDtypeStruct(direction.shape, f32),
            jax.ShapeDtypeStruct((ITERS, 1, lanes), f32),
        ),
        in_specs=[vmem] * 7,
        out_specs=(vmem,) * 3,
        scratch_shapes=[
            pltpu.VMEM((subs, rhs, dofs), f32),
            pltpu.VMEM((subs, rhs, dofs), f32),
            pltpu.VMEM((coarse if slots <= 12 else TILE, slots * wide), bf16),
            pltpu.VMEM((coarse // TILE, TILE, TILE), bf16),
            pltpu.VMEM((coarse // TILE, TILE, TILE), bf16),
            pltpu.VMEM((slots, 1, wide), jnp.int32),
            pltpu.VMEM((ITERS, n_mem, share, wide), f32),
            pltpu.VMEM((ITERS, slots, share, wide), f32),
            pltpu.VMEM((ITERS, slots, share, wide), f32),
            pltpu.VMEM((ITERS, slots, share, wide), f32),
            pltpu.VMEM((2 * ITERS + 1, total, 1, lanes), f32),
            pltpu.VMEM((1, lanes), f32),
            dma((1,)), dma((1,)),
            dma((ITERS,)), dma((ITERS,)), dma((ITERS,)), dma((ITERS,)),
            dma((2 * ITERS + 1,)), dma((2 * ITERS + 1,)),
        ],
        compiler_params=pltpu.CompilerParams(has_side_effects=True, vmem_limit_bytes=62 * 2**20),
    )(residual, direction, local_inverse, dirichlet, cpad, cmap, coarse_factor[0])
    return res, direc, steps[:, 0, :rhs]


def solution(mesh):
    return jax.shard_map(
        functools.partial(local, mesh.shape["grp"], mesh.shape["mem"]),
        mesh=mesh,
        in_specs=(
            P(("grp", "mem"), None, None),
            P(("grp", "mem"), None, None),
            P(("grp", "mem"), None, None),
            P(("grp", "mem"), None, None),
            P(("grp", "mem"), None, None),
            P(("grp", "mem"), None),
            P("grp", None, None),
        ),
        out_specs=(P(("grp", "mem"), None, None), P(("grp", "mem"), None, None), P()),
        check_vma=False,
    )
```

```python
import functools

import jax
import jax.numpy as jnp
from jax import lax
from jax.experimental import pallas as pl
from jax.experimental.pallas import tpu as pltpu
from jax.sharding import PartitionSpec as P

ITERS = 3
TILE = 256
GROUP = 4
MESH = pl.DeviceIdType.MESH
f32, bf16 = jnp.float32, jnp.bfloat16


def nn(a, b):
    return lax.dot_general(a, b, (((1,), (0,)), ((), ())), preferred_element_type=f32)


def nt(a, b):
    return lax.dot_general(a, b, (((1,), (1,)), ((), ())), preferred_element_type=f32)


def split(x):
    high = x.astype(bf16)
    return high, (x - high.astype(f32)).astype(bf16)


def stacked(x):
    return jnp.concatenate(split(x), axis=0)


def folded(x):
    half = x.shape[0] // 2
    return x[:half] + x[half:]


def invert_blocks(factor_ref, inv_high, inv_low):
    count = factor_ref.shape[0] // TILE
    together = GROUP if count % GROUP == 0 else 1
    half = TILE // 2
    rows = lax.broadcasted_iota(jnp.int32, (TILE, TILE), 0)
    cols = lax.broadcasted_iota(jnp.int32, (TILE, TILE), 1)

    def below(size):
        return (rows // size == cols // size + 1) & ((rows // size) % 2 == 1)

    def product(x, c):
        xh, xl = split(x[0])
        t = nn(c, xh) + nn(c, xl)
        th, tl = split(t)
        xh, xl = split(x[1])
        return nn(xh, th) + (nn(xh, tl) + nn(xl, th))

    def some(step, carry):
        tiles, found = [], []
        for k in range(together):
            at = pl.multiple_of((step * together + k) * TILE, TILE)
            tile = factor_ref[pl.ds(at, TILE), pl.ds(at, TILE)].astype(f32)
            diagonal = jnp.where(rows == cols, tile, 0.0)
            by_row = 1.0 / jnp.sum(diagonal, axis=1, keepdims=True)
            by_col = 1.0 / jnp.sum(diagonal, axis=0, keepdims=True)
            first = jnp.where(below(1), -by_row * tile * by_col, 0.0)
            tiles.append(tile)
            found.append(jnp.where(rows == cols, by_row, first))
        size = 2
        while size < half:
            mask = below(size)
            for k in range(together):
                c = jnp.where(mask, tiles[k], 0.0).astype(bf16)
                found[k] = found[k] - product((found[k], found[k]), c)
            size *= 2
        for k in range(together):
            x = found[k]
            upper, lower = x[:half, :half], x[half:, half:]
            corner = -product((upper, lower), tiles[k][half:, :half].astype(bf16))
            x = jnp.concatenate([x[:half], jnp.concatenate([corner, lower], axis=1)], axis=0)
            xh, xl = split(x)
            inv_high[step * together + k] = xh
            inv_low[step * together + k] = xl
        return carry

    lax.fori_loop(0, count // together, some, 0)


def coarse_solve(loads, factor_ref, inv_high, inv_low):
    count = len(loads)

    def part(i, j):
        return factor_ref[i * TILE : (i + 1) * TILE, j * TILE : (j + 1) * TILE]

    loads = list(loads)
    for i in range(count):
        b = stacked(loads[i])
        loads[i] = folded(nt(b, inv_high[i]) + nt(b, inv_low[i]))
        x = stacked(loads[i])
        for j in range(i + 1, count):
            loads[j] = loads[j] - folded(nt(x, part(j, i)))
    for i in reversed(range(count)):
        b = stacked(loads[i])
        loads[i] = folded(nn(b, inv_high[i]) + nn(b, inv_low[i]))
        x = stacked(loads[i])
        for j in reversed(range(i)):
            loads[j] = loads[j] - folded(nn(x, part(i, j)))
    return loads


def kernel(
    n_grp, n_mem,
    res_in, dir_in, linv, dirich, cpad, cmap, factor_in,
    res, direc, steps,
    pre, image, change, onehot, factor, inv_high, inv_low, load_p, load_d,
    cm_recv, p_send, p_recv, k_send, k_recv, sums, norm,
    f_s, cm_s, cm_r, p_s, p_r, k_s, k_r, a_s, a_r,
):
    subs, rhs, dofs = res_in.shape
    wide = cpad.shape[1]
    coarse = factor.shape[0]
    lanes = sums.shape[3]
    share = p_send.shape[2]
    last = steps.shape[0] - 1
    total = n_grp * n_mem
    slots = 3 * n_mem
    grp, mem = lax.axis_index("grp"), lax.axis_index("mem")
    me = grp * n_mem + mem
    mine = n_mem + mem
    eye = lax.broadcasted_iota(jnp.int32, (rhs, lanes), 0) == lax.broadcasted_iota(jnp.int32, (rhs, lanes), 1)

    eye_share = lax.broadcasted_iota(jnp.int32, (share, lanes), 1) == mem * share + lax.broadcasted_iota(
        jnp.int32, (share, lanes), 0
    )

    def to_row(column):
        return jnp.sum(jnp.where(eye, column, 0.0), axis=0, keepdims=True)

    def to_share(row):
        return jnp.sum(jnp.where(eye_share, row, 0.0), axis=1, keepdims=True)

    def to_column(row):
        return jnp.sum(jnp.where(eye, row, 0.0), axis=1, keepdims=True)

    def wait_bytes(ref, *sems):
        for sem in sems:
            pltpu.make_async_copy(ref, ref, sem).wait()

    def to_owners(source, target, send_sem, recv_sem):
        def one(d, carry):
            slot = (mine + d) % slots
            shift, other = slot // n_mem, slot % n_mem
            pltpu.make_async_remote_copy(
                src_ref=source(other), dst_ref=target(shift * n_mem + mem),
                send_sem=send_sem, recv_sem=recv_sem,
                device_id=((grp + shift + n_grp - 1) % n_grp, other), device_id_type=MESH,
            ).start()
            return carry

        lax.fori_loop(1, slots, one, 0)

    def to_users(source, target, send_sem, recv_sem):
        def one(d, carry):
            slot = (mine + d) % slots
            shift, other = slot // n_mem, slot % n_mem
            pltpu.make_async_remote_copy(
                src_ref=source(slot), dst_ref=target(shift * n_mem + mem),
                send_sem=send_sem, recv_sem=recv_sem,
                device_id=((grp + n_grp + 1 - shift) % n_grp, other), device_id_type=MESH,
            ).start()
            return carry

        lax.fori_loop(1, slots, one, 0)

    def sum_start(r, products):
        columns = [to_row(jnp.sum(x, axis=1, keepdims=True)) for x in products]
        columns += [jnp.zeros((1, lanes), f32)] * (4 - len(columns))
        sums[r, me] = jnp.concatenate(columns, axis=0)

        def one(d, carry):
            to = (me + d) % total
            pltpu.make_async_remote_copy(
                src_ref=sums.at[r, me], dst_ref=sums.at[r, me],
                send_sem=a_s.at[r], recv_sem=a_r.at[r],
                device_id=(to // n_mem, to % n_mem), device_id_type=MESH,
            ).start()
            return carry

        lax.fori_loop(1, total, one, 0)

    def sum_finish(r):
        wait_bytes(sums.at[r, pl.ds(0, total - 1)], a_s.at[r], a_r.at[r])
        return jnp.sum(sums[r], axis=0)

    def partial_of(values):
        acc = jnp.zeros((2 * rhs, wide), f32)
        for s in range(subs):
            solved = folded(nn(stacked(values[s]), linv[s]))
            acc = acc + nt(stacked(solved), cpad[s])
        return folded(acc)

    def partial_start(r, values):
        p_send[r] = partial_of(values).reshape(p_send.shape[1:])
        to_owners(lambda other: p_send.at[r, other], lambda slot: p_recv.at[r, slot], p_s.at[r], p_r.at[r])
        p_recv[r, mine] = p_send[r, mem]

    def partial_finish(r):
        wait_bytes(p_recv.at[r, pl.ds(0, slots - 1)], p_s.at[r], p_r.at[r])

    factor_copy = pltpu.make_async_copy(factor_in, factor, f_s.at[0])
    factor_copy.start()
    to_owners(lambda other: cmap, lambda slot: cm_recv.at[slot], cm_s.at[0], cm_r.at[0])
    cm_recv[mine] = cmap[...]
    acc = jnp.zeros((rhs, dofs), f32)
    for s in range(subs):
        value = res_in[s]
        out = folded(nn(stacked(value), dirich[s]))
        res[s] = value
        direc[s] = dir_in[s]
        pre[s] = out
        acc = acc + value * out
    sum_start(0, [acc])
    partial_start(0, direc)
    partial_start(1, pre)
    factor_copy.wait()
    invert_blocks(factor, inv_high, inv_low)
    wait_bytes(cm_recv.at[pl.ds(0, slots - 1)], cm_s.at[0], cm_r.at[0])
    held = onehot.shape[0] == coarse
    place = lax.broadcasted_iota(jnp.int32, (TILE, wide), 0)

    def fill(start, at):
        for slot in range(slots):
            row = cm_recv[slot] - coarse * (slot // n_mem) - start
            onehot[pl.ds(at, TILE), slot * wide : (slot + 1) * wide] = jnp.where(place == row, 1.0, 0.0).astype(bf16)

    def rows_of(i):
        if held:
            return onehot[i * TILE : (i + 1) * TILE, :]
        fill(i * TILE, 0)
        return onehot[...]

    if held:
        def fill_one(i, carry):
            at = pl.multiple_of(i * TILE, TILE)
            fill(at, at)
            return carry

        lax.fori_loop(0, coarse // TILE, fill_one, 0)
    def scattered(rounds):
        packed = jnp.concatenate(
            [jnp.concatenate([stacked(p_recv[r, slot]) for slot in range(slots)], axis=1) for r in rounds], axis=0
        )
        for i in range(coarse // TILE):
            out = nt(packed, rows_of(i))
            yield i * TILE, [folded(out[2 * share * k : 2 * share * (k + 1)]) for k in range(len(rounds))]

    partial_finish(0)
    partial_finish(1)
    for at, (first, second) in scattered((0, 1)):
        load_d[:, at : at + TILE] = first
        load_p[:, at : at + TILE] = second
    norm[...] = sum_finish(0)[0:1]

    def iteration(t, carry):
        loads = [load_d[:, at : at + TILE] for at in range(0, coarse, TILE)]
        loads = coarse_solve(loads, factor, inv_high, inv_low)
        if held:
            packed = jnp.concatenate([stacked(x) for x in loads], axis=1)
            for slot in range(slots):
                k_send[t, slot] = folded(nn(packed, onehot[:, slot * wide : (slot + 1) * wide]))
        else:
            wanted = sum(folded(nn(stacked(x), rows_of(i))) for i, x in enumerate(loads))
            for slot in range(slots):
                k_send[t, slot] = wanted[:, slot * wide : (slot + 1) * wide]
        to_users(lambda slot: k_send.at[t, slot], lambda slot: k_recv.at[t, slot], k_s.at[t], k_r.at[t])
        k_recv[t, mine] = k_send[t, mine]
        wait_bytes(k_recv.at[t, pl.ds(0, slots - 1)], k_s.at[t], k_r.at[t])
        got = k_recv[t].reshape(3, rhs, wide)
        picked = stacked(got[0] + got[1] + got[2])
        zero = jnp.zeros((rhs, dofs), f32)
        curve, cross, square = zero, zero, zero
        for s in range(subs):
            now = direc[s]
            lifted = folded(nn(picked, cpad[s]))
            out = nn((now + lifted).astype(bf16), linv[s])
            image[s] = out
            curve = curve + now * out
            moved = folded(nn(stacked(out), dirich[s]))
            change[s] = moved
            cross = cross + out * pre[s]
            square = square + out * moved
        sum_start(t + 1, [curve, cross, square])

        @pl.when(t < last)
        def _():
            partial_start(t + 2, change)

        norm_now = norm[...]
        summed = sum_finish(t + 1)
        alpha = norm_now / summed[0:1]
        norm_next = norm_now - alpha * (2.0 * summed[1:2] - alpha * summed[2:3])
        beta = norm_next / norm_now
        steps[t] = alpha
        norm[...] = norm_next
        by_alpha, by_beta = to_column(alpha), to_column(beta)
        for s in range(subs):
            res[s] = res[s] - by_alpha * image[s]
            new = pre[s] - by_alpha * change[s]
            pre[s] = new
            direc[s] = new + by_beta * direc[s]

        @pl.when(t < last)
        def _():
            share_alpha, share_beta = to_share(alpha), to_share(beta)
            partial_finish(t + 2)
            for at, (moved,) in scattered((t + 2,)):
                new = load_p[:, at : at + TILE] - share_alpha * moved
                load_p[:, at : at + TILE] = new
                load_d[:, at : at + TILE] = new + share_beta * load_d[:, at : at + TILE]

        return carry

    lax.fori_loop(0, last + 1, iteration, 0)


def local(n_grp, n_mem, residual, direction, local_inverse, dirichlet, coupling, corner_map, coarse_factor):
    subs, rhs, dofs = residual.shape
    corners = coupling.shape[1]
    coarse = coarse_factor.shape[1]
    used = subs * corners
    wide = -(-used // TILE) * TILE
    lanes = -(-rhs // 128) * 128
    total, slots, share = n_grp * n_mem, 3 * n_mem, rhs // n_mem
    own = jnp.arange(wide) // corners
    tiled = jnp.pad(jnp.tile(coupling, (1, subs, 1)), ((0, 0), (0, wide - used), (0, 0)))
    cpad = jnp.where(own[None, :, None] == jnp.arange(subs)[:, None, None], tiled, 0).astype(bf16)
    cmap = jnp.pad(corner_map.reshape(1, used), ((0, 0), (0, wide - used)), constant_values=-1)
    vmem = pl.BlockSpec(memory_space=pltpu.VMEM)
    dma = pltpu.SemaphoreType.DMA
    res, direc, steps = pl.pallas_call(
        functools.partial(kernel, n_grp, n_mem),
        out_shape=(
            jax.ShapeDtypeStruct(residual.shape, f32),
            jax.ShapeDtypeStruct(direction.shape, f32),
            jax.ShapeDtypeStruct((ITERS, 1, lanes), f32),
        ),
        in_specs=[vmem] * 6 + [pl.BlockSpec(memory_space=pl.ANY)],
        out_specs=(vmem,) * 3,
        scratch_shapes=[
            pltpu.VMEM((subs, rhs, dofs), f32),
            pltpu.VMEM((subs, rhs, dofs), f32),
            pltpu.VMEM((subs, rhs, dofs), f32),
            pltpu.VMEM((coarse if slots <= 12 else TILE, slots * wide), bf16),
            pltpu.VMEM((coarse, coarse), bf16),
            pltpu.VMEM((coarse // TILE, TILE, TILE), bf16),
            pltpu.VMEM((coarse // TILE, TILE, TILE), bf16),
            pltpu.VMEM((share, coarse), f32),
            pltpu.VMEM((share, coarse), f32),
            pltpu.VMEM((slots, 1, wide), jnp.int32),
            pltpu.VMEM((ITERS + 1, n_mem, share, wide), f32),
            pltpu.VMEM((ITERS + 1, slots, share, wide), f32),
            pltpu.VMEM((ITERS, slots, share, wide), f32),
            pltpu.VMEM((ITERS, slots, share, wide), f32),
            pltpu.VMEM((ITERS + 1, total, 4, lanes), f32),
            pltpu.VMEM((1, lanes), f32),
            dma((1,)), dma((1,)), dma((1,)),
            dma((ITERS + 1,)), dma((ITERS + 1,)), dma((ITERS,)), dma((ITERS,)),
            dma((ITERS + 1,)), dma((ITERS + 1,)),
        ],
        compiler_params=pltpu.CompilerParams(has_side_effects=True, vmem_limit_bytes=62 * 2**20),
    )(residual, direction, local_inverse, dirichlet, cpad, cmap, coarse_factor[0])
    return res, direc, steps[:, 0, :rhs]


def solution(mesh):
    return jax.shard_map(
        functools.partial(local, mesh.shape["grp"], mesh.shape["mem"]),
        mesh=mesh,
        in_specs=(
            P(("grp", "mem"), None, None),
            P(("grp", "mem"), None, None),
            P(("grp", "mem"), None, None),
            P(("grp", "mem"), None, None),
            P(("grp", "mem"), None, None),
            P(("grp", "mem"), None),
            P("grp", None, None),
        ),
        out_specs=(P(("grp", "mem"), None, None), P(("grp", "mem"), None, None), P()),
        check_vma=False,
    )
```
